512 devices in a mesh: ladder: 16 (over y, z_lo), grp: 32 (over x, z_hi, core).
Axes of the slice: x: 4, y: 8, z: 8 (z_hi: 4, z_lo: 2; z = z_hi * 2 + z_lo), core: 2. Of those that a mesh axis runs over, the one named last changes fastest.
Arguments:
- init_up: int32 [8192, 144], P(('ladder', 'grp')), may hold values 0 or 1
- flip_site: int32 [4, 8192], P(None, ('ladder', 'grp')), may hold values from 0 to 143
- accept: int32 [4, 8192], P(None, ('ladder', 'grp')), may hold values from 0 to 1
- swap_ok: int32 [4, 8, 512], P(None, None, 'grp'), may hold values 0 or 1
- ladder_bit: int32 [4, 32], P(None, 'grp'), may hold values from 0 to 3
- w_embed: bfloat16 [4, 72], replicated, may hold values from -3 to 3
- pos_embed: float32 [36, 72], replicated, may hold values from -6 to 6
- w_value: bfloat16 [2, 72, 72], replicated, may hold values from -0.75 to 0.75
- mixing: float32 [2, 12, 36, 36], replicated, may hold values from -1 to 1
- w_out: bfloat16 [2, 72, 72], replicated, may hold values from -0.75 to 0.75
- w_in: bfloat16 [2, 72, 288], replicated, may hold values from -0.75 to 0.75
- w_back: bfloat16 [2, 288, 72], replicated, may hold values from -0.375 to 0.375
- w_final: float32 [72, 72], replicated, may hold values from -0.75 to 0.75
- b_final: float32 [72], replicated, may hold values from -5 to 5
Outputs:
- proposal_amp: float32 [4, 8192], P(None, ('ladder', 'grp'))
- final_spins: float32 [8192, 144], P(('ladder', 'grp'))
- final_amp: float32 [8192], P(('ladder', 'grp'))
- accept_counts: float32 [16, 4], P('ladder')
The draws below stay inside these ranges and needn't reach their ends.
All inputs are finite; a program needn't handle non-finite values. No bound on the sum of `init_up` or of `swap_ok` on one device may be relied on, other than what follows from the above.
Results may differ from the reference program's by a relative error of at most 0.002.
Values sent between devices are 32-bit elements; how exact they have to be, the bound alone decides.
No kernel may reach another device: no remote copies, remote signals or barrier semaphores. Data moves between devices by JAX's collectives and lax.ppermute only.
A program may use at most 64 MiB of HBM per device.

```python
import jax
import jax.numpy as jnp
from jax import lax

SIDE = 12
SITES = 144
PATCHES = 36
D = 72
HEADS = 12
HID = 288
LAYERS = 2
STEPS = 4
CHAINS_RUNG = 512
CHAINS = 8192
LADDER_BITS = 4
PAIRS = 8
N_LADDER = 16
N_GRP = 32


def draw_accept(key, part):
    chain_index = lax.broadcasted_iota(jnp.int32, (STEPS, CHAINS), 1) % CHAINS_RUNG
    threshold = 200 + 400 * chain_index // CHAINS_RUNG
    tickets = jax.random.randint(jax.random.fold_in(key, 11), (STEPS, CHAINS), 0, 1000)
    return (tickets < threshold).astype(jnp.int32)


def plant(entries, rng, low, largest):
    longest = entries.shape.index(max(entries.shape))
    spots = []
    for shift in (0, 1):
        where = [jax.random.randint(jax.random.fold_in(rng, axis), (), 0, length) for axis, length in enumerate(entries.shape)]
        where[longest] = (where[longest] + shift) % entries.shape[longest]
        spots.append(tuple(where))
    return entries.at[spots[0]].set(low).at[spots[1]].set(largest)


def noise(rng, dims, scale, limit, held_as=jnp.bfloat16):
    values = jax.random.normal(rng, dims, jnp.float32) * scale
    return jnp.minimum(jnp.maximum(values, -limit), limit).astype(held_as)


def setup_inputs(seed: int = 0) -> dict:
    arg_keys = jax.random.split(jax.random.key(seed), 15)
    init_up = plant((jax.random.randint(arg_keys[0], (CHAINS, SITES), 0, 2) < 1).astype(jnp.int32), jax.random.fold_in(arg_keys[0], 1), 0, 1)
    flip_site = plant(jax.random.randint(arg_keys[1], (STEPS, CHAINS), 0, SITES), jax.random.fold_in(arg_keys[1], 1), 0, SITES - 1).astype(jnp.int32)
    accept = draw_accept(jax.random.fold_in(arg_keys[14], 71), 0)
    swap_ok = plant((jax.random.randint(arg_keys[3], (STEPS, PAIRS, CHAINS_RUNG), 0, 2) < 1).astype(jnp.int32), jax.random.fold_in(arg_keys[3], 1), 0, 1)
    ladder_bit = plant(jax.random.randint(arg_keys[4], (STEPS, N_GRP), 0, LADDER_BITS), jax.random.fold_in(arg_keys[4], 1), 0, LADDER_BITS - 1).astype(jnp.int32)
    w_embed = noise(arg_keys[5], (4, D), 4 ** -0.5, 3.0)
    pos_embed = noise(arg_keys[6], (PATCHES, D), 1.0, 6.0, jnp.float32)
    w_value = noise(arg_keys[7], (LAYERS, D, D), D ** -0.5, 0.75)
    mixing = noise(arg_keys[8], (LAYERS, HEADS, PATCHES, PATCHES), PATCHES ** -0.5, 1.0, jnp.float32)
    w_out = noise(arg_keys[9], (LAYERS, D, D), D ** -0.5, 0.75)
    w_in = noise(arg_keys[10], (LAYERS, D, HID), D ** -0.5, 0.75)
    w_back = noise(arg_keys[11], (LAYERS, HID, D), HID ** -0.5, 0.375)
    w_final = noise(arg_keys[12], (D, D), D ** -0.5, 0.75, jnp.float32)
    b_final = noise(arg_keys[13], (D,), 1.0, 5.0, jnp.float32)
    return {"init_up": init_up, "flip_site": flip_site, "accept": accept, "swap_ok": swap_ok, "ladder_bit": ladder_bit, "w_embed": w_embed, "pos_embed": pos_embed, "w_value": w_value, "mixing": mixing, "w_out": w_out, "w_in": w_in, "w_back": w_back, "w_final": w_final, "b_final": b_final}


def layer_norm(values):
    center = values - lax.optimization_barrier(jnp.mean(values, axis=-1, keepdims=True))
    spread = lax.optimization_barrier(jnp.mean(center * center, axis=-1, keepdims=True))
    return center / jnp.sqrt(spread + 1e-05)

def log_cosh(values):
    return jnp.logaddexp(values, -values) - jnp.log(2.0)

def amplitude(spin_state, w_embed, pos_embed, w_value, mixing, w_out, w_in, w_back, w_final, b_final):
    chains = spin_state.shape[0]
    half_side = SIDE // 2
    patch_count = half_side * half_side
    patches = spin_state.reshape(chains, half_side, 2, half_side, 2).transpose(0, 1, 3, 2, 4).reshape(chains * patch_count, 4)
    stream = jnp.dot(patches, w_embed.astype(jnp.float32), precision=lax.Precision.HIGHEST)
    model_width = stream.shape[-1]
    stream = stream.reshape(chains, patch_count, model_width) + pos_embed
    head_count = mixing.shape[1]
    row_count = chains * patch_count
    for layer_index in range(w_value.shape[0]):
        normed = layer_norm(stream).astype(jnp.bfloat16).reshape(row_count, model_width)
        value_rows = jnp.dot(normed, w_value[layer_index], preferred_element_type=jnp.float32).astype(jnp.bfloat16)
        value_rows = value_rows.astype(jnp.float32).reshape(chains, patch_count, head_count, model_width // head_count)
        mixed_heads = jnp.einsum('hpq,nqhd->nphd', mixing[layer_index], value_rows, precision=lax.Precision.HIGHEST)
        mixed_heads = mixed_heads.astype(jnp.bfloat16).reshape(row_count, model_width)
        attended = jnp.dot(mixed_heads, w_out[layer_index], preferred_element_type=jnp.float32)
        stream = stream + attended.reshape(chains, patch_count, model_width)
        normed = layer_norm(stream).astype(jnp.bfloat16).reshape(row_count, model_width)
        hidden = jax.nn.gelu(jnp.dot(normed, w_in[layer_index], preferred_element_type=jnp.float32)).astype(jnp.bfloat16)
        backed = jnp.dot(hidden, w_back[layer_index], preferred_element_type=jnp.float32)
        stream = stream + backed.reshape(chains, patch_count, model_width)
    pooled = lax.optimization_barrier(jnp.sum(layer_norm(stream), axis=1)) / half_side
    head_values = jnp.dot(pooled, w_final, precision=lax.Precision.HIGHEST) + b_final
    return lax.optimization_barrier(jnp.mean(log_cosh(head_values), axis=-1))

def flipped(spin_state, sites):
    columns = lax.broadcasted_iota(jnp.int32, spin_state.shape, 1)
    return jnp.where(columns == sites[:, None].astype(jnp.int32), -spin_state, spin_state)

def reference(init_up, flip_site, accept, swap_ok, ladder_bit, w_embed, pos_embed, w_value, mixing, w_out, w_in, w_back, w_final, b_final):
    params = (w_embed, pos_embed, w_value, mixing, w_out, w_in, w_back, w_final, b_final)

    def rung_amplitudes(spin_state):
        blocks = spin_state.reshape(N_LADDER, CHAINS_RUNG, SITES)
        return lax.map(lambda rung_block: amplitude(rung_block, *params), blocks).reshape(CHAINS)
    spin_state = 2.0 * init_up.astype(jnp.float32) - 1.0
    log_amp = rung_amplitudes(spin_state)
    rungs = jnp.arange(N_LADDER, dtype=jnp.int32)
    per_block = CHAINS_RUNG // N_GRP
    proposals = []
    for step_index in range(STEPS):
        proposal = flipped(spin_state, flip_site[step_index])
        proposal_amp = rung_amplitudes(proposal)
        proposals.append(proposal_amp)
        taken = accept[step_index] == 1
        spin_state = jnp.where(taken[:, None], proposal, spin_state)
        log_amp = jnp.where(taken, proposal_amp, log_amp)
        block_stride = jnp.left_shift(jnp.int32(1), ladder_bit[step_index].astype(jnp.int32))
        place_stride = jnp.repeat(block_stride, per_block).astype(jnp.int32)
        partner = jnp.bitwise_xor(rungs[:, None], place_stride[None, :]).astype(jnp.int32)
        lower = jnp.minimum(rungs[:, None], partner)
        pair_index = (lower // (2 * place_stride[None, :]) * place_stride[None, :] + lower % place_stride[None, :]).astype(jnp.int32)
        decided = jnp.take_along_axis(swap_ok[step_index], pair_index, axis=0) == 1
        grouped = spin_state.reshape(N_LADDER, CHAINS_RUNG, SITES)
        partner_spins = jnp.take_along_axis(grouped, partner[:, :, None], axis=0)
        spin_state = jnp.where(decided[:, :, None], partner_spins, grouped).reshape(CHAINS, SITES)
        amp_grouped = log_amp.reshape(N_LADDER, CHAINS_RUNG)
        partner_amp = jnp.take_along_axis(amp_grouped, partner, axis=0)
        log_amp = jnp.where(decided, partner_amp, amp_grouped).reshape(CHAINS)
    counts = lax.optimization_barrier(jnp.sum(accept.reshape(STEPS, N_LADDER, CHAINS_RUNG), axis=2)).T.astype(jnp.float32)
    return (jnp.stack(proposals), spin_state, log_amp, counts)
```

```python
import jax
import jax.numpy as jnp
import numpy as np
from jax import lax
from jax.experimental import pallas as pl
from jax.experimental.pallas import tpu as pltpu
from jax.sharding import PartitionSpec as P

SIDE = 12
SITES = 144
PATCHES = 36
D = 72
HEADS = 12
HEAD_DIM = 6
HID = 288
LAYERS = 2
STEPS = 4
PAIRS = 8
RUNGS = 16
PLACES = 16

PACK = 7
LANES = 256
CHAINS = (STEPS + 1) * PLACES
GROUPS = -(-CHAINS // PACK)
ROWS = 96
SLOT = 8
HD = HEADS * SLOT
MSG = SITES + 2 * STEPS
GELU_A = float(np.sqrt(2.0 / np.pi))
GELU_B = GELU_A * 0.044715


def constants():
    lane = np.arange(LANES)
    used = lane < PACK * PATCHES
    patch = lane % PATCHES
    chain = lane // PATCHES
    spread = (np.arange(PATCHES)[:, None] == patch[None, :]) & used[None, :]
    block = (chain[:, None] == chain[None, :]) & used[:, None] & used[None, :]
    pick = np.zeros((SITES, 4 * LANES), np.float32)
    for row in range(2):
        for column in range(2):
            site = (2 * (patch // 6) + row) * SIDE + 2 * (patch % 6) + column
            pick[:, (row * 2 + column) * LANES : (row * 2 + column + 1) * LANES] = (
                np.arange(SITES)[:, None] == site[None, :]
            ) & used[None, :]
    pool = (chain[:, None] == np.arange(128)[None, :]) & used[:, None]
    pad = np.zeros((HD, D), np.float32)
    for head in range(HEADS):
        for entry in range(HEAD_DIM):
            pad[head * SLOT + entry, head * HEAD_DIM + entry] = 1.0
    repeat = np.zeros((4, 64), np.float32)
    for s in range(4):
        repeat[s, s * 16 : (s + 1) * 16] = 1.0
    low = jnp.bfloat16
    return (
        jnp.asarray(spread, low),
        jnp.asarray(spread.T, low),
        jnp.asarray(block, jnp.float32),
        jnp.asarray(pick, low),
        jnp.asarray(pool, low),
        jnp.asarray(pad, low),
        jnp.asarray(repeat, low),
    )


def mm(a, b):
    return jnp.dot(a, b, preferred_element_type=jnp.float32)


def mm_t(a, b):
    return lax.dot_general(a, b, (((1,), (1,)), ((), ())), preferred_element_type=jnp.float32)


def exact(a, b):
    return jnp.dot(a, b, preferred_element_type=jnp.float32, precision=lax.Precision.HIGHEST)


def norm(x):
    center = x - jnp.sum(x, axis=0, keepdims=True) * (1.0 / D)
    spread = jnp.sum(center * center, axis=0, keepdims=True) * (1.0 / D)
    return center * lax.rsqrt(spread + 1e-05)


def kernel(
    bit_ref,
    got_ref,
    swap_ref,
    w_embed_ref,
    pos_ref,
    w_value_ref,
    mixing_ref,
    w_out_ref,
    w_in_ref,
    w_back_ref,
    w_final_ref,
    b_final_ref,
    spread_ref,
    spread_t_ref,
    block_ref,
    pick_ref,
    pool_ref,
    pad_ref,
    repeat_ref,
    prop_ref,
    spins_ref,
    amp_ref,
    state,
    chains,
    picked,
    pos_x,
    embed_x,
    wv,
    wo,
    wi,
    wb,
    big,
    stream,
    value,
    mixed,
    pooled,
):
    low = jnp.bfloat16
    me = lax.axis_index("ladder")

    embed_x[...] = mm(w_embed_ref[...].astype(jnp.float32).T.astype(low), repeat_ref[...]).astype(low)
    pos_x[...] = exact(pos_ref[...].T, spread_ref[...].astype(jnp.float32))
    for layer in range(LAYERS):
        wv[layer] = mm_t(pad_ref[...], w_value_ref[layer]).astype(low)
        wo[layer] = mm(pad_ref[...], w_out_ref[layer]).T.astype(low)
        wi[layer] = w_in_ref[layer].astype(jnp.float32).T.astype(low)
        wb[layer] = w_back_ref[layer].astype(jnp.float32).T.astype(low)
        for head in range(HEADS):
            wide = mm(mixing_ref[layer, head].T.astype(low), spread_ref[...]).astype(low)
            big[layer, head] = (mm(spread_t_ref[...], wide) * block_ref[...]).astype(low)

    column = lax.broadcasted_iota(jnp.int32, (PLACES, SITES), 1).astype(jnp.float32)
    for rung in range(RUNGS):
        state[rung] = got_ref[rung, :, :SITES]
    chains[CHAINS:, :] = jnp.zeros((ROWS - CHAINS, SITES), jnp.float32)
    for step in range(STEPS):
        own_site = got_ref[me, :, SITES + step : SITES + step + 1]
        own = state[me]
        chains[step * PLACES : (step + 1) * PLACES, :] = jnp.where(column == own_site, -own, own)
        bit = bit_ref[step, 0]
        mask = jnp.left_shift(jnp.int32(1), bit)
        decided = swap_ref[step].T
        moved = []
        for rung in range(RUNGS):
            site = got_ref[rung, :, SITES + step : SITES + step + 1]
            taken = got_ref[rung, :, SITES + STEPS + step : SITES + STEPS + step + 1]
            flip = jnp.where(taken > 0.5, site, -1.0)
            now = state[rung]
            state[rung] = jnp.where(column == flip, -now, now)
        for pair in range(PAIRS):
            lower = jnp.left_shift(jnp.right_shift(jnp.int32(pair), bit), bit + 1) + jnp.bitwise_and(
                jnp.int32(pair), mask - 1
            )
            upper = lower + mask
            ok = decided[:, pair : pair + 1] == 1
            a, b = state[lower], state[upper]
            state[lower] = jnp.where(ok, b, a)
            state[upper] = jnp.where(ok, a, b)
    last = state[me]
    spins_ref[...] = last
    chains[STEPS * PLACES : CHAINS, :] = last

    picked[...] = mm(chains[...].astype(low), pick_ref[...])
    lane = lax.broadcasted_iota(jnp.int32, (16, LANES), 1)
    row = lax.broadcasted_iota(jnp.int32, (16, LANES), 0)
    slot = sum((lane >= PATCHES * k).astype(jnp.int32) for k in range(1, PACK + 1))

    def to_value(layer, group, x):
        projected = mm(wv[layer], norm(x).astype(low))
        for head in range(HEADS):
            value[head, group * SLOT : (group + 1) * SLOT, :] = projected[head * SLOT : (head + 1) * SLOT, :]

    for group in range(GROUPS):
        first = PACK * group // 8 * 8
        mine = slot + (PACK * group - first) == row
        parts = [
            jnp.where(mine, picked[first : first + 16, s * LANES : (s + 1) * LANES], 0.0) for s in range(4)
        ]
        x = mm(embed_x[...], jnp.concatenate(parts, axis=0).astype(low)) + pos_x[...]
        stream[group] = x
        to_value(0, group, x)

    pooled[...] = jnp.zeros_like(pooled)
    for layer in range(LAYERS):
        for head in range(HEADS):
            out = mm(value[head].astype(low), big[layer, head])
            for group in range(GROUPS):
                mixed[group, head * SLOT : (head + 1) * SLOT, :] = out[group * SLOT : (group + 1) * SLOT, :]
        for group in range(GROUPS):
            x = stream[group] + mm(wo[layer], mixed[group].astype(low))
            h = mm(wi[layer], norm(x).astype(low))
            h = h + h * jnp.tanh(h * (GELU_B * (h * h) + GELU_A))
            x = x + 0.5 * mm(wb[layer], h.astype(low))
            if layer + 1 < LAYERS:
                stream[group] = x
                to_value(layer + 1, group, x)
            else:
                x = norm(x)
                high = x.astype(low)
                rest = (x - high.astype(jnp.float32)).astype(low)
                total = mm(high, pool_ref[...]) + mm(rest, pool_ref[...])
                pooled[...] += total if group == 0 else pltpu.roll(total, PACK * group, 1)

    eye = lax.broadcasted_iota(jnp.int32, (D, D), 0) == lax.broadcasted_iota(jnp.int32, (D, D), 1)
    bias = jnp.sum(jnp.where(eye, b_final_ref[...], 0.0), axis=1, keepdims=True)
    heads = exact(w_final_ref[...].T, pooled[...] * (2.0 / SIDE)) + bias
    size = jnp.abs(heads)
    log_cosh = size + jnp.log1p(jnp.exp(-2.0 * size)) - float(np.log(2.0))
    amps = jnp.sum(log_cosh, axis=0, keepdims=True) * (1.0 / D)
    for step in range(STEPS):
        prop_ref[step : step + 1, :] = amps[:, step * PLACES : (step + 1) * PLACES]
    amp_ref[...] = amps[:, STEPS * PLACES : CHAINS]


def from_everyone(shard, axis):
    size = lax.axis_size(axis)
    return lax.all_to_all(
        jnp.broadcast_to(shard[None], (size, *shard.shape)), axis, 0, 0, tiled=True
    )


def on_device(
    init_up,
    flip_site,
    accept,
    swap_ok,
    ladder_bit,
    w_embed,
    pos_embed,
    w_value,
    mixing,
    w_out,
    w_in,
    w_back,
    w_final,
    b_final,
):
    f32, low = jnp.float32, jnp.bfloat16
    message = jnp.concatenate(
        [2.0 * init_up.astype(f32) - 1.0, flip_site.T.astype(f32), accept.T.astype(f32)], axis=1
    )
    got = from_everyone(message, "ladder")
    got = got.reshape(RUNGS, PLACES, MSG)
    local_counts = jnp.sum(accept, axis=1).astype(f32)
    vmem = pl.BlockSpec(memory_space=pltpu.VMEM)
    prop, spins, amp = pl.pallas_call(
        kernel,
        out_shape=(
            jax.ShapeDtypeStruct((STEPS, PLACES), f32),
            jax.ShapeDtypeStruct((PLACES, SITES), f32),
            jax.ShapeDtypeStruct((1, PLACES), f32),
        ),
        in_specs=[pl.BlockSpec(memory_space=pltpu.SMEM)] + [vmem] * 18,
        out_specs=(vmem, vmem, vmem),
        scratch_shapes=[
            pltpu.VMEM((RUNGS, PLACES, SITES), f32),
            pltpu.VMEM((ROWS, SITES), f32),
            pltpu.VMEM((ROWS, 4 * LANES), f32),
            pltpu.VMEM((D, LANES), f32),
            pltpu.VMEM((D, 64), low),
            pltpu.VMEM((LAYERS, HD, D), low),
            pltpu.VMEM((LAYERS, D, HD), low),
            pltpu.VMEM((LAYERS, HID, D), low),
            pltpu.VMEM((LAYERS, D, HID), low),
            pltpu.VMEM((LAYERS, HEADS, LANES, LANES), low),
            pltpu.VMEM((GROUPS, D, LANES), f32),
            pltpu.VMEM((HEADS, ROWS, LANES), f32),
            pltpu.VMEM((GROUPS, HD, LANES), f32),
            pltpu.VMEM((D, 128), f32),
        ],
        compiler_params=pltpu.CompilerParams(vmem_limit_bytes=40 * 1024 * 1024),
        cost_estimate=pl.CostEstimate(flops=2 * 10**9, bytes_accessed=10**6, transcendentals=10**6),
    )(
        ladder_bit,
        got,
        swap_ok,
        w_embed,
        pos_embed,
        w_value,
        mixing,
        w_out,
        w_in,
        w_back,
        w_final,
        b_final.reshape(1, D),
        *constants(),
    )
    totals = from_everyone(local_counts, "grp").sum(axis=0)
    return (prop, spins, amp.reshape(PLACES), totals.reshape(1, -1))


def solution(mesh):
    placed = (
        P(("ladder", "grp"), None),
        P(None, ("ladder", "grp")),
        P(None, ("ladder", "grp")),
        P(None, None, "grp"),
        P(None, "grp"),
        P(),
        P(),
        P(),
        P(),
        P(),
        P(),
        P(),
        P(),
        P(),
    )
    return jax.shard_map(
        on_device,
        mesh=mesh,
        in_specs=placed,
        out_specs=(
            P(None, ("ladder", "grp")),
            P(("ladder", "grp"), None),
            P(("ladder", "grp")),
            P("ladder", None),
        ),
        check_vma=False,
    )
```

```python
import jax
import jax.numpy as jnp
import numpy as np
from jax import lax
from jax.experimental import pallas as pl
from jax.experimental.pallas import tpu as pltpu
from jax.sharding import PartitionSpec as P


SIDE = 12
SITES = 144
PATCHES = 36
D = 72
HEADS = 12
HEAD_DIM = 6
HID = 288
LAYERS = 2
STEPS = 4
PAIRS = 8
RUNGS = 16
PLACES = 16

PACK = 7
LANES = 256
CHAINS = (STEPS + 1) * PLACES
GROUPS = -(-CHAINS // PACK)
ROWS = 96
SLOT = 8
HD = HEADS * SLOT
MSG = SITES + 2 * STEPS
GELU_A = float(np.sqrt(2.0 / np.pi))
GELU_B = GELU_A * 0.044715


def constants():
    lane = np.arange(LANES)
    used = lane < PACK * PATCHES
    patch = lane % PATCHES
    chain = lane // PATCHES
    spread = (np.arange(PATCHES)[:, None] == patch[None, :]) & used[None, :]
    block = (chain[:, None] == chain[None, :]) & used[:, None] & used[None, :]
    pick = np.zeros((SITES, 4 * LANES), np.float32)
    for row in range(2):
        for column in range(2):
            site = (2 * (patch // 6) + row) * SIDE + 2 * (patch % 6) + column
            pick[:, (row * 2 + column) * LANES : (row * 2 + column + 1) * LANES] = (
                np.arange(SITES)[:, None] == site[None, :]
            ) & used[None, :]
    pool = (chain[:, None] == np.arange(128)[None, :]) & used[:, None]
    pad = np.zeros((HD, D), np.float32)
    for head in range(HEADS):
        for entry in range(HEAD_DIM):
            pad[head * SLOT + entry, head * HEAD_DIM + entry] = 1.0
    repeat = np.zeros((4, 64), np.float32)
    for s in range(4):
        repeat[s, s * 16 : (s + 1) * 16] = 1.0
    low = jnp.bfloat16
    return (
        jnp.asarray(spread, low),
        jnp.asarray(spread.T, low),
        jnp.asarray(block, jnp.float32),
        jnp.asarray(pick, low),
        jnp.asarray(pool, low),
        jnp.asarray(pad, low),
        jnp.asarray(repeat, low),
    )


def mm(a, b):
    return jnp.dot(a, b, preferred_element_type=jnp.float32)


def mm_t(a, b):
    return lax.dot_general(a, b, (((1,), (1,)), ((), ())), preferred_element_type=jnp.float32)


def exact(a, b):
    return jnp.dot(a, b, preferred_element_type=jnp.float32, precision=lax.Precision.HIGHEST)


def norm(x):
    center = x - jnp.sum(x, axis=0, keepdims=True) * (1.0 / D)
    spread = jnp.sum(center * center, axis=0, keepdims=True) * (1.0 / D)
    return center * lax.rsqrt(spread + 1e-05)


def kernel(
    bit_hbm,
    got_ref,
    swap_ref,
    small_ref,
    pos_ref,
    w_value_ref,
    mixing_ref,
    w_out_ref,
    w_in_ref,
    w_back_ref,
    w_final_ref,
    spread_ref,
    spread_t_ref,
    block_ref,
    pick_ref,
    pool_ref,
    pad_ref,
    repeat_ref,
    prop_ref,
    spins_ref,
    amp_ref,
    state,
    chains,
    picked,
    pos_x,
    embed_x,
    wv,
    wo,
    wi,
    wb,
    big,
    stream,
    normed,
    rests,
    hidden,
    value,
    mixed,
    bit_ref,
    arrived,
):
    low = jnp.bfloat16
    me = lax.axis_index("ladder")
    copy = pltpu.make_async_copy(bit_hbm, bit_ref, arrived)
    copy.start()

    pos_x[...] = exact(pos_ref[...].T, spread_ref[...].astype(jnp.float32))
    for layer in range(LAYERS):
        wv[layer] = mm_t(pad_ref[...], w_value_ref[layer]).astype(low)
        wo[layer] = mm(pad_ref[...], w_out_ref[layer]).T.astype(low)
        wi[layer] = w_in_ref[layer].astype(jnp.float32).T.astype(low)
        wb[layer] = (0.5 * w_back_ref[layer].astype(jnp.float32)).T.astype(low)
    for layer in range(LAYERS):
        for head in range(HEADS):
            one = mixing_ref[layer, head]
            twice = jnp.concatenate([one, one], axis=1).T.astype(low)
            wide = mm(twice, spread_ref[...])
            for half in range(2):
                lanes = slice(half * 128, half * 128 + 128)
                tiles = []
                for start in range(0, LANES, 2 * PATCHES):
                    rows = min(2 * PATCHES, LANES - start)
                    end = min(start + 2 * PATCHES, PACK * PATCHES)
                    if end <= half * 128 or start >= half * 128 + 128:
                        tiles.append(jnp.zeros((rows, 128), jnp.float32))
                    else:
                        tiles.append(wide[:rows, lanes] * block_ref[start : start + rows, lanes])
                big[layer, head, :, lanes] = jnp.concatenate(tiles, axis=0).astype(low)

    copy.wait()
    embed_x[...] = mm(small_ref[:4].T.astype(low), repeat_ref[...]).astype(low)

    column = lax.broadcasted_iota(jnp.int32, (PLACES, SITES), 1).astype(jnp.float32)
    for rung in range(RUNGS):
        state[rung] = got_ref[rung, :, :SITES]
    chains[CHAINS:, :] = jnp.zeros((ROWS - CHAINS, SITES), jnp.float32)
    for step in range(STEPS):
        own_site = got_ref[me, :, SITES + step : SITES + step + 1]
        own = state[me]
        chains[step * PLACES : (step + 1) * PLACES, :] = jnp.where(column == own_site, -own, own)
        bit = bit_ref[step, 0]
        mask = jnp.left_shift(jnp.int32(1), bit)
        decided = swap_ref[step].T
        for rung in range(RUNGS):
            site = got_ref[rung, :, SITES + step : SITES + step + 1]
            taken = got_ref[rung, :, SITES + STEPS + step : SITES + STEPS + step + 1]
            flip = jnp.where(taken > 0.5, site, -1.0)
            now = state[rung]
            state[rung] = jnp.where(column == flip, -now, now)
        for pair in range(PAIRS):
            lower = jnp.left_shift(jnp.right_shift(jnp.int32(pair), bit), bit + 1) + jnp.bitwise_and(
                jnp.int32(pair), mask - 1
            )
            upper = lower + mask
            ok = decided[:, pair : pair + 1] == 1
            a, b = state[lower], state[upper]
            state[lower] = jnp.where(ok, b, a)
            state[upper] = jnp.where(ok, a, b)
    last = state[me]
    spins_ref[...] = last
    chains[STEPS * PLACES : CHAINS, :] = last

    picked[...] = mm(chains[...].astype(low), pick_ref[...])
    lane = lax.broadcasted_iota(jnp.int32, (16, LANES), 1)
    row = lax.broadcasted_iota(jnp.int32, (16, LANES), 0)
    slot = sum((lane >= PATCHES * k).astype(jnp.int32) for k in range(1, PACK + 1))

    def to_value(layer):
        for pair in range(GROUPS // 2):
            one = mm(wv[layer], normed[2 * pair])
            two = mm(wv[layer], normed[2 * pair + 1])
            for head in range(HEADS):
                rows = slice(head * SLOT, (head + 1) * SLOT)
                both = jnp.concatenate([one[rows], two[rows]], axis=0)
                value[head, pair * 2 * SLOT : (pair + 1) * 2 * SLOT, :] = both.astype(low)

    def mix(layer):
        for pair in range(HEADS // 2):
            one = mm(value[2 * pair], big[layer, 2 * pair])
            two = mm(value[2 * pair + 1], big[layer, 2 * pair + 1])
            for group in range(GROUPS):
                rows = slice(group * SLOT, (group + 1) * SLOT)
                both = jnp.concatenate([one[rows], two[rows]], axis=0)
                mixed[group, pair * 2 * SLOT : (pair + 1) * 2 * SLOT, :] = both.astype(low)

    for group in range(GROUPS):
        first = PACK * group // 8 * 8
        mine = slot + (PACK * group - first) == row
        parts = [
            jnp.where(mine, picked[first : first + 16, s * LANES : (s + 1) * LANES], 0.0) for s in range(4)
        ]
        x = mm(embed_x[...], jnp.concatenate(parts, axis=0).astype(low)) + pos_x[...]
        stream[group] = x
        normed[group] = norm(x).astype(low)

    for layer in range(LAYERS):
        to_value(layer)
        mix(layer)
        for group in range(GROUPS):
            x = stream[group] + mm(wo[layer], mixed[group])
            stream[group] = x
            normed[group] = norm(x).astype(low)
        for group in range(GROUPS):
            h = mm(wi[layer], normed[group]).astype(low)
            hidden[group] = h + h * jnp.tanh(h * (low(GELU_B) * (h * h) + low(GELU_A)))
        for group in range(GROUPS):
            x = stream[group] + mm(wb[layer], hidden[group])
            if layer + 1 < LAYERS:
                stream[group] = x
                normed[group] = norm(x).astype(low)
            else:
                x = norm(x)
                high = x.astype(low)
                normed[group] = high
                rests[group] = (x - high.astype(jnp.float32)).astype(low)
    total = jnp.zeros((D, 128), jnp.float32)
    for group in range(GROUPS):
        part = mm(normed[group], pool_ref[...]) + mm(rests[group], pool_ref[...])
        total = total + (part if group == 0 else pltpu.roll(part, PACK * group, 1))

    eye = lax.broadcasted_iota(jnp.int32, (D, D), 0) == lax.broadcasted_iota(jnp.int32, (D, D), 1)
    bias = jnp.sum(jnp.where(eye, small_ref[4:5], 0.0), axis=1, keepdims=True)
    heads = exact(w_final_ref[...].T, total * (2.0 / SIDE)) + bias
    size = jnp.abs(heads)
    log_cosh = size + jnp.log1p(jnp.exp(-2.0 * size)) - float(np.log(2.0))
    amps = jnp.sum(log_cosh, axis=0, keepdims=True) * (1.0 / D)
    for step in range(STEPS):
        prop_ref[step : step + 1, :] = amps[:, step * PLACES : (step + 1) * PLACES]
    amp_ref[...] = amps[:, STEPS * PLACES : CHAINS]


def from_everyone(shard, axis):
    size = lax.axis_size(axis)
    return lax.all_to_all(
        jnp.broadcast_to(shard[None], (size, *shard.shape)), axis, 0, 0, tiled=True
    )


def on_device(
    init_up,
    flip_site,
    accept,
    swap_ok,
    ladder_bit,
    w_embed,
    pos_embed,
    w_value,
    mixing,
    w_out,
    w_in,
    w_back,
    w_final,
    b_final,
):
    f32, low = jnp.float32, jnp.bfloat16
    marks = jnp.concatenate([flip_site, accept], axis=0).astype(f32).T
    message = jnp.concatenate([2.0 * init_up.astype(f32) - 1.0, marks], axis=1)
    got = from_everyone(message, "ladder")
    got = got.reshape(RUNGS, PLACES, MSG)
    local_counts = jnp.sum(accept.astype(f32), axis=1)
    vmem = pl.BlockSpec(memory_space=pltpu.VMEM)
    hbm = pl.BlockSpec(memory_space=pltpu.HBM)
    replay = pl.pallas_call(
        kernel,
        out_shape=(
            jax.ShapeDtypeStruct((STEPS, PLACES), f32),
            jax.ShapeDtypeStruct((PLACES, SITES), f32),
            jax.ShapeDtypeStruct((1, PLACES), f32),
        ),
        in_specs=[hbm] + [vmem] * 17,
        out_specs=(vmem, vmem, vmem),
        scratch_shapes=[
            pltpu.VMEM((RUNGS, PLACES, SITES), f32),
            pltpu.VMEM((ROWS, SITES), f32),
            pltpu.VMEM((ROWS, 4 * LANES), f32),
            pltpu.VMEM((D, LANES), f32),
            pltpu.VMEM((D, 64), low),
            pltpu.VMEM((LAYERS, HD, D), low),
            pltpu.VMEM((LAYERS, D, HD), low),
            pltpu.VMEM((LAYERS, HID, D), low),
            pltpu.VMEM((LAYERS, D, HID), low),
            pltpu.VMEM((LAYERS, HEADS, LANES, LANES), low),
            pltpu.VMEM((GROUPS, D, LANES), f32),
            pltpu.VMEM((GROUPS, D, LANES), low),
            pltpu.VMEM((GROUPS, D, LANES), low),
            pltpu.VMEM((GROUPS, HID, LANES), low),
            pltpu.VMEM((HEADS, ROWS, LANES), low),
            pltpu.VMEM((GROUPS, HD, LANES), low),
            pltpu.SMEM((STEPS, 1), jnp.int32),
            pltpu.SemaphoreType.DMA,
        ],
        compiler_params=pltpu.CompilerParams(vmem_limit_bytes=40 * 1024 * 1024),
        cost_estimate=pl.CostEstimate(flops=2 * 10**9, bytes_accessed=10**6, transcendentals=10**6),
    )
    small = jnp.concatenate([w_embed.astype(f32), b_final[None]], axis=0)
    inputs = (
        ladder_bit,
        got,
        swap_ok,
        small,
        pos_embed,
        w_value,
        mixing,
        w_out,
        w_in,
        w_back,
        w_final,
        *constants(),
    )
    prop, spins, amp = replay(*inputs)
    size = lax.axis_size("grp")
    other = lax.ppermute(local_counts, "grp", [(g, g ^ 1) for g in range(size)])
    both = local_counts + other
    shares = jnp.broadcast_to(both[None, None], (size // 2, 1, STEPS))
    groups = [list(range(core, size, 2)) for core in range(2)]
    shares = lax.all_to_all(shares, "grp", 0, 0, tiled=True, axis_index_groups=groups)
    totals = shares.sum(axis=(0, 1))
    return (prop, spins, amp.reshape(PLACES), totals.reshape(1, -1))


def solution(mesh):
    placed = (
        P(("ladder", "grp"), None),
        P(None, ("ladder", "grp")),
        P(None, ("ladder", "grp")),
        P(None, None, "grp"),
        P(None, "grp"),
        P(),
        P(),
        P(),
        P(),
        P(),
        P(),
        P(),
        P(),
        P(),
    )
    return jax.shard_map(
        on_device,
        mesh=mesh,
        in_specs=placed,
        out_specs=(
            P(None, ("ladder", "grp")),
            P(("ladder", "grp"), None),
            P(("ladder", "grp")),
            P("ladder", None),
        ),
        check_vma=False,
    )
```

```python
import jax
import jax.numpy as jnp
import numpy as np
from jax import lax
from jax.experimental import pallas as pl
from jax.experimental.pallas import tpu as pltpu
from jax.sharding import PartitionSpec as P


SIDE = 12
SITES = 144
PATCHES = 36
D = 72
HEADS = 12
HEAD_DIM = 6
HID = 288
LAYERS = 2
STEPS = 4
PAIRS = 8
RUNGS = 16
PLACES = 16

PACK = 7
LANES = 256
CHAINS = (STEPS + 1) * PLACES
GROUPS = -(-CHAINS // PACK)
ROWS = 96
SLOT = 8
HD = HEADS * SLOT
TAIL = SITES - 128 + 2 * STEPS
GELU_A = float(np.sqrt(2.0 / np.pi))
GELU_B = GELU_A * 0.044715


def constants():
    lane = np.arange(LANES)
    used = lane < PACK * PATCHES
    patch = lane % PATCHES
    chain = lane // PATCHES
    spread = (np.arange(PATCHES)[:, None] == patch[None, :]) & used[None, :]
    block = (chain[:, None] == chain[None, :]) & used[:, None] & used[None, :]
    pick = np.zeros((SITES, 4 * LANES), np.float32)
    for row in range(2):
        for column in range(2):
            site = (2 * (patch // 6) + row) * SIDE + 2 * (patch % 6) + column
            pick[:, (row * 2 + column) * LANES : (row * 2 + column + 1) * LANES] = (
                np.arange(SITES)[:, None] == site[None, :]
            ) & used[None, :]
    pad = np.zeros((HD, D), np.float32)
    for head in range(HEADS):
        for entry in range(HEAD_DIM):
            pad[head * SLOT + entry, head * HEAD_DIM + entry] = 1.0
    low = jnp.bfloat16
    return (
        jnp.asarray(spread, low),
        jnp.asarray(block, jnp.float32),
        jnp.asarray(pick, low),
        jnp.asarray(pad, low),
    )


def mm(a, b):
    return jnp.dot(a, b, preferred_element_type=jnp.float32)


def mm_t(a, b):
    return lax.dot_general(a, b, (((1,), (1,)), ((), ())), preferred_element_type=jnp.float32)


def exact(a, b):
    return jnp.dot(a, b, preferred_element_type=jnp.float32, precision=lax.Precision.HIGHEST)


def norm(x):
    center = x - jnp.sum(x, axis=0, keepdims=True) * (1.0 / D)
    spread = jnp.sum(center * center, axis=0, keepdims=True) * (1.0 / D)
    return center * lax.rsqrt(spread + 1e-05)


def compose(up_hbm, site_hbm, accept_hbm, message_ref, up_ref, site_ref, accept_ref, arrived):
    f32 = jnp.float32
    copies = [
        pltpu.make_async_copy(up_hbm, up_ref, arrived.at[0]),
        pltpu.make_async_copy(site_hbm, site_ref, arrived.at[1]),
        pltpu.make_async_copy(accept_hbm, accept_ref, arrived.at[2]),
    ]
    for copy in copies:
        copy.start()
    for copy in copies:
        copy.wait()
    marks = jnp.concatenate([site_ref[...], accept_ref[...]], axis=0).astype(f32).T
    spins = 2.0 * up_ref[...].astype(f32) - 1.0
    rest = jnp.concatenate(
        [spins[:, 128:], marks, jnp.zeros((PLACES, 128 - TAIL), f32)], axis=1
    )
    tail = rest[:4]
    for k in range(1, 4):
        tail = tail + pltpu.roll(rest[4 * k : 4 * k + 4], 32 * k, 1)
    for rung in range(RUNGS):
        for k in range(4):
            message_ref[rung, :, k * 128 : (k + 1) * 128] = spins[4 * k : 4 * k + 4, :128]
        message_ref[rung, :, 512:] = tail


def kernel(
    bit_hbm,
    sent_ref,
    swap_ref,
    small_ref,
    pos_ref,
    w_value_ref,
    mixing_ref,
    w_out_ref,
    w_in_ref,
    w_back_ref,
    w_final_ref,
    spread_ref,
    block_ref,
    pick_ref,
    pad_ref,
    prop_ref,
    spins_ref,
    amp_ref,
    state,
    chains,
    picked,
    pos_x,
    embed_x,
    wv,
    wo,
    wi,
    wb,
    big,
    stream,
    normed,
    rests,
    hidden,
    value,
    mixed,
    got_ref,
    bit_ref,
    arrived,
):
    low = jnp.bfloat16
    me = lax.axis_index("ladder")
    copy = pltpu.make_async_copy(bit_hbm, bit_ref, arrived)
    copy.start()

    pos_x[...] = exact(pos_ref[...].T, spread_ref[...].astype(jnp.float32))
    for layer in range(LAYERS):
        wv[layer] = mm_t(pad_ref[...], w_value_ref[layer]).astype(low)
        wo[layer] = mm(pad_ref[...], w_out_ref[layer]).T.astype(low)
        wi[layer] = w_in_ref[layer].astype(jnp.float32).T.astype(low)
        wb[layer] = (0.5 * w_back_ref[layer].astype(jnp.float32)).astype(low)
    for layer in range(LAYERS):
        for head in range(HEADS):
            one = mixing_ref[layer, head]
            twice = jnp.concatenate([one, one], axis=1).T.astype(low)
            wide = mm(twice, spread_ref[...])
            for half in range(2):
                lanes = slice(half * 128, half * 128 + 128)
                tiles = []
                for start in range(0, LANES, 2 * PATCHES):
                    rows = min(2 * PATCHES, LANES - start)
                    end = min(start + 2 * PATCHES, PACK * PATCHES)
                    if end <= half * 128 or start >= half * 128 + 128:
                        tiles.append(jnp.zeros((rows, 128), jnp.float32))
                    else:
                        tiles.append(wide[:rows, lanes] * block_ref[start : start + rows, lanes])
                big[layer, head, :, lanes] = jnp.concatenate(tiles, axis=0).astype(low)

    copy.wait()
    repeat = lax.broadcasted_iota(jnp.int32, (4, 64), 1) // 16 == lax.broadcasted_iota(jnp.int32, (4, 64), 0)
    repeat = repeat.astype(jnp.float32).astype(low)
    embed_x[...] = mm(small_ref[:4].T.astype(low), repeat).astype(low)

    column = lax.broadcasted_iota(jnp.int32, (PLACES, SITES), 1).astype(jnp.float32)
    for rung in range(RUNGS):
        tail = sent_ref[rung, :, 512:]
        tails = [tail] + [pltpu.roll(tail, 128 - 32 * k, 1) for k in range(1, 4)]
        heads = [sent_ref[rung, :, k * 128 : (k + 1) * 128] for k in range(4)]
        got_ref[rung, :, :128] = jnp.concatenate(heads, axis=0)
        got_ref[rung, :, 128:] = jnp.concatenate(tails, axis=0)
        state[rung] = got_ref[rung, :, :SITES]
    chains[CHAINS:, :] = jnp.zeros((ROWS - CHAINS, SITES), jnp.float32)
    for step in range(STEPS):
        own_site = got_ref[me, :, SITES + step : SITES + step + 1]
        own = state[me]
        chains[step * PLACES : (step + 1) * PLACES, :] = jnp.where(column == own_site, -own, own)
        bit = bit_ref[0, step]
        mask = jnp.left_shift(jnp.int32(1), bit)
        decided = swap_ref[step].T
        for rung in range(RUNGS):
            site = got_ref[rung, :, SITES + step : SITES + step + 1]
            taken = got_ref[rung, :, SITES + STEPS + step : SITES + STEPS + step + 1]
            flip = jnp.where(taken > 0.5, site, -1.0)
            now = state[rung]
            state[rung] = jnp.where(column == flip, -now, now)
        for pair in range(PAIRS):
            lower = jnp.left_shift(jnp.right_shift(jnp.int32(pair), bit), bit + 1) + jnp.bitwise_and(
                jnp.int32(pair), mask - 1
            )
            upper = lower + mask
            ok = decided[:, pair : pair + 1] == 1
            a, b = state[lower], state[upper]
            state[lower] = jnp.where(ok, b, a)
            state[upper] = jnp.where(ok, a, b)
    last = state[me]
    spins_ref[...] = last
    chains[STEPS * PLACES : CHAINS, :] = last

    picked[...] = mm(chains[...].astype(low), pick_ref[...])
    lane = lax.broadcasted_iota(jnp.int32, (16, LANES), 1)
    row = lax.broadcasted_iota(jnp.int32, (16, LANES), 0)
    slot = sum((lane >= PATCHES * k).astype(jnp.int32) for k in range(1, PACK + 1))

    def to_value(layer):
        for pair in range(GROUPS // 2):
            one = mm(wv[layer], normed[2 * pair])
            two = mm(wv[layer], normed[2 * pair + 1])
            for head in range(HEADS):
                rows = slice(head * SLOT, (head + 1) * SLOT)
                both = jnp.concatenate([one[rows], two[rows]], axis=0)
                value[head, pair * 2 * SLOT : (pair + 1) * 2 * SLOT, :] = both.astype(low)

    def mix(layer):
        for pair in range(HEADS // 2):
            one = mm(value[2 * pair], big[layer, 2 * pair])
            two = mm(value[2 * pair + 1], big[layer, 2 * pair + 1])
            for group in range(GROUPS):
                rows = slice(group * SLOT, (group + 1) * SLOT)
                both = jnp.concatenate([one[rows], two[rows]], axis=0)
                mixed[group, pair * 2 * SLOT : (pair + 1) * 2 * SLOT, :] = both.astype(low)

    for group in range(GROUPS):
        first = PACK * group // 8 * 8
        mine = slot + (PACK * group - first) == row
        parts = [
            jnp.where(mine, picked[first : first + 16, s * LANES : (s + 1) * LANES], 0.0) for s in range(4)
        ]
        x = mm(embed_x[...], jnp.concatenate(parts, axis=0).astype(low)) + pos_x[...]
        stream[group] = x
        normed[group] = norm(x).astype(low)

    for layer in range(LAYERS):
        to_value(layer)
        mix(layer)
        for group in range(GROUPS):
            x = stream[group] + mm(wo[layer], mixed[group])
            stream[group] = x
            normed[group] = norm(x).astype(low)
        for group in range(GROUPS):
            h = mm(wi[layer], normed[group]).astype(low)
            hidden[group] = h + h * jnp.tanh(h * (low(GELU_B) * (h * h) + low(GELU_A)))
        for group in range(GROUPS):
            x = stream[group] + mm(wb[layer], hidden[group])
            if layer + 1 < LAYERS:
                stream[group] = x
                normed[group] = norm(x).astype(low)
            else:
                x = norm(x)
                high = x.astype(low)
                normed[group] = high
                rests[group] = (x - high.astype(jnp.float32)).astype(low)
    slots = lax.broadcasted_iota(jnp.int32, (LANES, 128), 1)
    patch = lax.broadcasted_iota(jnp.int32, (LANES, 128), 0) - PATCHES * slots
    pool = jnp.where((patch >= 0) & (patch < PATCHES) & (slots < PACK), 1.0, 0.0).astype(low)
    total = jnp.zeros((D, 128), jnp.float32)
    for group in range(GROUPS):
        part = mm(normed[group], pool) + mm(rests[group], pool)
        total = total + (part if group == 0 else pltpu.roll(part, PACK * group, 1))

    eye = lax.broadcasted_iota(jnp.int32, (D, D), 0) == lax.broadcasted_iota(jnp.int32, (D, D), 1)
    bias = jnp.sum(jnp.where(eye, small_ref[4:5], 0.0), axis=1, keepdims=True)
    heads = exact(w_final_ref[...].T, total * (2.0 / SIDE)) + bias
    size = jnp.abs(heads)
    log_cosh = size + jnp.log1p(jnp.exp(-2.0 * size)) - float(np.log(2.0))
    amps = jnp.sum(log_cosh, axis=0, keepdims=True) * (1.0 / D)
    for step in range(STEPS):
        prop_ref[step : step + 1, :] = amps[:, step * PLACES : (step + 1) * PLACES]
    amp_ref[...] = amps[:, STEPS * PLACES : CHAINS]


def on_device(
    init_up,
    flip_site,
    accept,
    swap_ok,
    ladder_bit,
    w_embed,
    pos_embed,
    w_value,
    mixing,
    w_out,
    w_in,
    w_back,
    w_final,
    b_final,
):
    f32, low = jnp.float32, jnp.bfloat16
    vmem = pl.BlockSpec(memory_space=pltpu.VMEM)
    message = pl.pallas_call(
        compose,
        out_shape=jax.ShapeDtypeStruct((RUNGS, 4, 640), f32),
        in_specs=[pl.BlockSpec(memory_space=pltpu.HBM)] * 3,
        out_specs=vmem,
        scratch_shapes=[
            pltpu.VMEM((PLACES, SITES), jnp.int32),
            pltpu.VMEM((STEPS, PLACES), jnp.int32),
            pltpu.VMEM((STEPS, PLACES), jnp.int32),
            pltpu.SemaphoreType.DMA((3,)),
        ],
        compiler_params=pltpu.CompilerParams(vmem_limit_bytes=67000000),
    )(init_up, flip_site, accept)
    got = lax.all_to_all(message, "ladder", 0, 0, tiled=True)
    local_counts = jnp.sum(accept.astype(f32), axis=1)
    vmem = pl.BlockSpec(memory_space=pltpu.VMEM)
    hbm = pl.BlockSpec(memory_space=pltpu.HBM)
    replay = pl.pallas_call(
        kernel,
        out_shape=(
            jax.ShapeDtypeStruct((STEPS, PLACES), f32),
            jax.ShapeDtypeStruct((PLACES, SITES), f32),
            jax.ShapeDtypeStruct((1, PLACES), f32),
        ),
        in_specs=[hbm] + [vmem] * 14,
        out_specs=(vmem, vmem, vmem),
        scratch_shapes=[
            pltpu.VMEM((RUNGS, PLACES, SITES), f32),
            pltpu.VMEM((ROWS, SITES), f32),
            pltpu.VMEM((ROWS, 4 * LANES), f32),
            pltpu.VMEM((D, LANES), f32),
            pltpu.VMEM((D, 64), low),
            pltpu.VMEM((LAYERS, HD, D), low),
            pltpu.VMEM((LAYERS, D, HD), low),
            pltpu.VMEM((LAYERS, HID, D), low),
            pltpu.VMEM((LAYERS, D, HID), low),
            pltpu.VMEM((LAYERS, HEADS, LANES, LANES), low),
            pltpu.VMEM((GROUPS, D, LANES), f32),
            pltpu.VMEM((GROUPS, D, LANES), low),
            pltpu.VMEM((GROUPS, D, LANES), low),
            pltpu.VMEM((GROUPS, HID, LANES), low),
            pltpu.VMEM((HEADS, ROWS, LANES), low),
            pltpu.VMEM((GROUPS, HD, LANES), low),
            pltpu.VMEM((RUNGS, PLACES, 256), f32),
            pltpu.SMEM((1, STEPS), jnp.int32),
            pltpu.SemaphoreType.DMA,
        ],
        compiler_params=pltpu.CompilerParams(vmem_limit_bytes=40 * 1024 * 1024),
        cost_estimate=pl.CostEstimate(flops=2 * 10**9, bytes_accessed=10**6, transcendentals=10**6),
    )
    small = jnp.concatenate([w_embed.astype(f32), b_final[None]], axis=0)
    inputs = (
        ladder_bit.T,
        got,
        swap_ok,
        small,
        pos_embed,
        w_value,
        mixing,
        w_out,
        w_in,
        jnp.swapaxes(w_back, 1, 2),
        w_final,
        *constants(),
    )
    prop, spins, amp = replay(*inputs)
    size = lax.axis_size("grp")
    other = lax.ppermute(local_counts, "grp", [(g, g ^ 1) for g in range(size)])
    both = local_counts + other
    shares = jnp.broadcast_to(both[None, None], (size // 2, 1, STEPS))
    groups = [list(range(core, size, 2)) for core in range(2)]
    shares = lax.all_to_all(shares, "grp", 0, 0, tiled=True, axis_index_groups=groups)
    totals = shares.sum(axis=(0, 1))
    return (prop, spins, amp.reshape(PLACES), totals.reshape(1, -1))


def solution(mesh):
    placed = (
        P(("ladder", "grp"), None),
        P(None, ("ladder", "grp")),
        P(None, ("ladder", "grp")),
        P(None, None, "grp"),
        P(None, "grp"),
        P(),
        P(),
        P(),
        P(),
        P(),
        P(),
        P(),
        P(),
        P(),
    )
    return jax.shard_map(
        on_device,
        mesh=mesh,
        in_specs=placed,
        out_specs=(
            P(None, ("ladder", "grp")),
            P(("ladder", "grp"), None),
            P(("ladder", "grp")),
            P("ladder", None),
        ),
        check_vma=False,
    )
```
